32 devices in a mesh: dp: 4 (over y, z), cp: 8 (over x, core).
Axes of the slice: x: 4, y: 2, z: 2, core: 2. Of those that a mesh axis runs over, the one named last changes fastest.
The devices are a block of a 4x4x8 slice.
Arguments:
- latents: bfloat16 [8, 128, 128, 16], P('dp', 'cp'), parts along dimension 0
- w_in: bfloat16 [3, 3, 16, 512], replicated
- b_in: bfloat16 [512], replicated
- w_conv: bfloat16 [4, 3, 3, 512, 512], replicated
- b_conv: bfloat16 [4, 512], replicated
- gn_scale: bfloat16 [5, 512], replicated
- gn_shift: bfloat16 [5, 512], replicated
- w_attn: bfloat16 [4, 512, 512], replicated
- b_attn: bfloat16 [4, 512], replicated
Outputs:
- output: bfloat16 [8, 128, 128, 512], P('dp', 'cp'), parts along dimension 0
There are 4 independent parts. The reference program is written for one: setup_inputs(seed, part) draws one part's arguments, and reference() takes and returns one part's arrays. A program takes and returns all parts, laid end to end along the dimension named above; an argument that names none is the same for every part.
All inputs are finite; a program needn't handle non-finite values.
Results may differ from the reference program's by a relative error of at most 0.02.
Values are sent between devices in bfloat16 or wider.
A program may use at most 768 MiB of HBM per device.

```python
import jax
import jax.numpy as jnp
from jax import lax

SAMPLES = 2
LAT_H = 128
LAT_W = 128
Z_CH = 16
CHANNELS = 512
GROUPS = 32
QUERY_TOKENS = 1024
GN_EPS = 1e-6


def setup_inputs(seed: int = 0, part: int = 0) -> dict:
    root_key = jax.random.key(seed)
    rand_keys = jax.random.split(root_key, 9)
    lat_keys = jax.random.split(jax.random.fold_in(rand_keys[0], part), 4)
    lat_noise = jax.random.normal(lat_keys[0], (SAMPLES, LAT_H, LAT_W, Z_CH), jnp.float32)
    row_pos = (2.0 * jnp.arange(LAT_H, dtype=jnp.float32) / (LAT_H - 1) - 1.0).reshape(1, LAT_H, 1, 1)
    row_slope = 0.8 * jax.random.normal(lat_keys[1], (SAMPLES, 1, 1, Z_CH), jnp.float32)
    row_scale = jax.random.uniform(lat_keys[2], (SAMPLES, LAT_H, 1, 1), jnp.float32, 0.6, 1.4)
    row_shift = 0.3 * jax.random.normal(lat_keys[3], (SAMPLES, LAT_H, 1, Z_CH), jnp.float32)
    latents = lat_noise * row_scale + row_slope * row_pos + row_shift
    attn_gain = jnp.array([2.4, 2.4, 1.0, 1.0], dtype=jnp.float32).reshape(4, 1, 1)
    w_in = jax.random.normal(rand_keys[1], (3, 3, Z_CH, CHANNELS), jnp.float32) * (9 * Z_CH) ** -0.5
    b_in = 0.5 * jax.random.normal(rand_keys[2], (CHANNELS,), jnp.float32)
    w_conv = jax.random.normal(rand_keys[3], (4, 3, 3, CHANNELS, CHANNELS), jnp.float32) * (9 * CHANNELS) ** -0.5
    b_conv = 0.3 * jax.random.normal(rand_keys[4], (4, CHANNELS), jnp.float32)
    gn_scale = 1.0 + 0.3 * jax.random.normal(rand_keys[5], (5, CHANNELS), jnp.float32)
    gn_shift = 0.3 * jax.random.normal(rand_keys[6], (5, CHANNELS), jnp.float32)
    w_attn = jax.random.normal(rand_keys[7], (4, CHANNELS, CHANNELS), jnp.float32) * attn_gain * CHANNELS ** -0.5
    b_attn = 0.3 * jax.random.normal(rand_keys[8], (4, CHANNELS), jnp.float32)
    return {
        'latents': latents.astype(jnp.bfloat16),
        'w_in': w_in.astype(jnp.bfloat16),
        'b_in': b_in.astype(jnp.bfloat16),
        'w_conv': w_conv.astype(jnp.bfloat16),
        'b_conv': b_conv.astype(jnp.bfloat16),
        'gn_scale': gn_scale.astype(jnp.bfloat16),
        'gn_shift': gn_shift.astype(jnp.bfloat16),
        'w_attn': w_attn.astype(jnp.bfloat16),
        'b_attn': b_attn.astype(jnp.bfloat16),
    }


def conv3x3(x_val, weight, conv_bias):
    conv_out = lax.conv_general_dilated(x_val.astype(jnp.float32), weight.astype(jnp.float32), (1, 1), 'SAME', dimension_numbers=('NHWC', 'HWIO', 'NHWC'))
    return conv_out + conv_bias.astype(jnp.float32)


def group_norm(x_val, norm_gain, norm_bias):
    n_batch, n_rows, n_width, n_chan = x_val.shape
    grouped = x_val.astype(jnp.float32).reshape(n_batch, n_rows, n_width, GROUPS, n_chan // GROUPS)
    grp_mean = jnp.mean(grouped, axis=(1, 2, 4), keepdims=True)
    centered = grouped - grp_mean
    grp_var = jnp.mean(jnp.square(centered), axis=(1, 2, 4), keepdims=True)
    normed = (centered * lax.rsqrt(grp_var + GN_EPS)).reshape(x_val.shape)
    return normed * norm_gain.astype(jnp.float32) + norm_bias.astype(jnp.float32)


def resnet_block(h_val, w_conv, b_conv, gn_scale, gn_shift, conv_idx, norm_idx):
    act_in = jax.nn.silu(group_norm(h_val, gn_scale[norm_idx], gn_shift[norm_idx])).astype(jnp.bfloat16)
    mid_act = conv3x3(act_in, w_conv[conv_idx], b_conv[conv_idx]).astype(jnp.bfloat16)
    act_two = jax.nn.silu(group_norm(mid_act, gn_scale[norm_idx + 1], gn_shift[norm_idx + 1])).astype(jnp.bfloat16)
    conv_two = conv3x3(act_two, w_conv[conv_idx + 1], b_conv[conv_idx + 1])
    return (h_val.astype(jnp.float32) + conv_two).astype(jnp.bfloat16)


def attention(h_val, w_attn, b_attn, norm_gain, norm_bias):
    n_batch, n_rows, n_width, n_chan = h_val.shape
    normed = group_norm(h_val, norm_gain, norm_bias).astype(jnp.bfloat16).reshape(-1, n_chan)

    def project(j_idx):
        proj = jnp.dot(normed, w_attn[j_idx], preferred_element_type=jnp.float32) + b_attn[j_idx].astype(jnp.float32)
        return proj.astype(jnp.bfloat16).reshape(n_batch, n_rows * n_width, n_chan)

    queries = project(0)
    keys_all = project(1)
    vals_all = project(2)
    block_rows = max([divisor for divisor in range(1, n_rows + 1) if n_rows % divisor == 0 and divisor * n_width <= QUERY_TOKENS] + [1])
    n_blocks = n_rows // block_rows
    att_scale = n_chan ** -0.5

    def one_sample(operands):
        q_sample, k_sample, v_sample = operands

        def one_block(q_block):
            scores = jnp.dot(q_block, k_sample.T, preferred_element_type=jnp.float32) * att_scale
            attn_prob = jax.nn.softmax(scores, axis=-1).astype(jnp.bfloat16)
            return jnp.dot(attn_prob, v_sample, preferred_element_type=jnp.float32).astype(jnp.bfloat16)

        return lax.map(one_block, q_sample.reshape(n_blocks, block_rows * n_width, n_chan))

    attended = lax.map(one_sample, (queries, keys_all, vals_all)).reshape(-1, n_chan)
    proj_out = jnp.dot(attended, w_attn[3], preferred_element_type=jnp.float32) + b_attn[3].astype(jnp.float32)
    return (h_val.astype(jnp.float32) + proj_out.reshape(h_val.shape)).astype(jnp.bfloat16)


def reference(latents, w_in, b_in, w_conv, b_conv, gn_scale, gn_shift, w_attn, b_attn):
    hidden = conv3x3(latents, w_in, b_in).astype(jnp.bfloat16)
    hidden = resnet_block(hidden, w_conv, b_conv, gn_scale, gn_shift, 0, 0)
    hidden = attention(hidden, w_attn, b_attn, gn_scale[2], gn_shift[2])
    hidden = resnet_block(hidden, w_conv, b_conv, gn_scale, gn_shift, 2, 3)
    return hidden
```

```python
import functools

import jax
import jax.numpy as jnp
from jax import lax
from jax.experimental import pallas as pl
from jax.experimental.pallas import tpu as pltpu
from jax.sharding import PartitionSpec as P

GROUPS = 32
GN_EPS = 1e-6
LOG2E = 1.4426950408889634
MESH = pl.DeviceIdType.MESH
F32, BF16 = jnp.float32, jnp.bfloat16
ANY = pl.BlockSpec(memory_space=pl.ANY)
VMEM = pl.BlockSpec(memory_space=pltpu.VMEM)
SMEM = pl.BlockSpec(memory_space=pltpu.SMEM)
MIB = 1024 * 1024


def peer(n_dev, offset):
    return {'cp': lax.rem(lax.axis_index('cp') + 2 * offset + n_dev, n_dev)}


def add_stats(st_ref, yf):
    y3 = yf.reshape(yf.shape[0] // 8, 8, yf.shape[1])
    st_ref[0:8, :] += jnp.sum(y3, axis=0)
    st_ref[8:16, :] += jnp.sum(y3 * y3, axis=0)


def conv_in_kernel(n_blk, p_ref, w_ref, b_ref, y_ref, st_ref):
    m = y_ref.shape[0] // n_blk
    st_ref[...] = jnp.zeros_like(st_ref)

    def body(i, _):
        off = pl.multiple_of(i * m, m)
        acc = lax.dot_general(p_ref[:, pl.ds(off, m)], w_ref[...], (((0,), (0,)), ((), ())), preferred_element_type=F32)
        y = (acc + b_ref[...]).astype(BF16)
        y_ref[pl.ds(off, m), :] = y
        yf = y.astype(F32)
        add_stats(st_ref, yf)
        return 0

    lax.fori_loop(0, n_blk, body, 0)


def conv_in(patches, w2, bias):
    tok, ch = patches.shape[1], w2.shape[1]
    return pl.pallas_call(
        functools.partial(conv_in_kernel, 8),
        out_shape=(jax.ShapeDtypeStruct((tok, ch), BF16), jax.ShapeDtypeStruct((16, ch), F32)),
        in_specs=[VMEM] * 3,
        out_specs=(VMEM, VMEM),
        name='conv_in',
        compiler_params=pltpu.CompilerParams(vmem_limit_bytes=24 * MIB),
    )(patches, w2, bias)


def exchange_kernel(n_dev, count, width, x_ref, st_ref, gain_ref, aff_ref, top_ref, bot_ref, sbuf, send_sem, recv_sem):
    tok = x_ref.shape[0]
    n_chip = n_dev // 2
    barrier = pltpu.get_barrier_semaphore()
    for d in range(1, n_chip):
        pl.semaphore_signal(barrier, inc=1, device_id=peer(n_dev, d), device_id_type=MESH)
    pl.semaphore_wait(barrier, n_chip - 1)
    copies = []
    copies.append(pltpu.make_async_remote_copy(
        x_ref.at[pl.ds(tok - width, width)], top_ref, send_sem.at[0], recv_sem.at[0], device_id=peer(n_dev, 1), device_id_type=MESH))
    copies.append(pltpu.make_async_remote_copy(
        x_ref.at[pl.ds(0, width)], bot_ref, send_sem.at[1], recv_sem.at[1], device_id=peer(n_dev, -1), device_id_type=MESH))
    stats = [pltpu.make_async_remote_copy(
        st_ref, sbuf.at[d - 1], send_sem.at[1 + d], recv_sem.at[1 + d], device_id=peer(n_dev, d), device_id_type=MESH)
        for d in range(1, n_chip)]
    for c in stats + copies:
        c.start()
    tot = st_ref[...]
    for c in stats:
        c.wait()
    for d in range(1, n_chip):
        tot = tot + sbuf[d - 1]
    ch = tot.shape[1]
    lane = lax.broadcasted_iota(jnp.int32, tot.shape, 1)
    k = 1
    while k < ch // GROUPS:
        tot = tot + jnp.where((lane & k) != 0, pltpu.roll(tot, k, 1), pltpu.roll(tot, ch - k, 1))
        k *= 2
    tot = tot * (1.0 / count)
    mean, square = tot[0:8, :], tot[8:16, :]
    for k in (1, 2, 4):
        mean = mean + pltpu.roll(mean, k, 0)
        square = square + pltpu.roll(square, k, 0)
    aff_ref[0:8, :] = mean
    aff_ref[8:16, :] = lax.rsqrt(square - mean * mean + GN_EPS) * gain_ref[0:8, :]
    aff_ref[16:24, :] = gain_ref[8:16, :]
    for c in copies:
        c.wait()


def exchange(n_dev, width, x, st, gain):
    tok, ch = x.shape
    n_chip = n_dev // 2
    count = tok * n_chip * (ch // GROUPS)
    return pl.pallas_call(
        functools.partial(exchange_kernel, n_dev, count, width),
        out_shape=(jax.ShapeDtypeStruct((24, ch), F32), jax.ShapeDtypeStruct((width, ch), BF16), jax.ShapeDtypeStruct((width, ch), BF16)),
        in_specs=[ANY, VMEM, VMEM],
        out_specs=(VMEM, VMEM, VMEM),
        scratch_shapes=[
            pltpu.VMEM((n_chip - 1, 16, ch), F32),
            pltpu.SemaphoreType.DMA((n_chip + 1,)),
            pltpu.SemaphoreType.DMA((n_chip + 1,)),
        ],
        name='exchange',
        compiler_params=pltpu.CompilerParams(collective_id=0, has_side_effects=True, vmem_limit_bytes=8 * MIB),
    )(x, st, gain)


def conv_kernel(width, n_rows, blk_rows, has_res, *refs):
    if has_res:
        (x_ref, top_ref, bot_ref, edge_ref, aff_ref, w_ref, b_ref, r_ref, y_ref, st_ref,
         xs, u3, ws, ys, rs, x_sem, w_sem, y_sem, r_sem) = refs
    else:
        (x_ref, top_ref, bot_ref, edge_ref, aff_ref, w_ref, b_ref, y_ref, st_ref,
         xs, u3, ws, ys, x_sem, w_sem, y_sem) = refs
    ch = x_ref.shape[1]
    n_blk = n_rows // blk_rows
    m = blk_rows * width
    x_in = [pltpu.make_async_copy(x_ref.at[pl.ds(b * m, m)], xs.at[pl.ds(b * m, m)], x_sem.at[b]) for b in range(n_blk)]
    for c in x_in:
        c.start()
    w_in = [pltpu.make_async_copy(w_ref.at[d], ws.at[d], w_sem.at[d]) for d in range(3)]
    for c in w_in:
        c.start()
    if has_res:
        r_in = pltpu.make_async_copy(r_ref, rs, r_sem.at[0])
        r_in.start()
    mean, scale, shift = aff_ref[0:1, :], aff_ref[8:9, :], aff_ref[16:17, :]
    rows = lax.broadcasted_iota(jnp.int32, (width, ch), 0)

    def prep(v, row, keep=None):
        t = (v.astype(F32) - mean) * scale + shift
        u = t / (1.0 + jnp.exp(-t))
        if keep is not None:
            u = jnp.where(keep, u, 0.0)
        off = pl.multiple_of(row * width, width)
        u3[pl.ds(off, width), 0:ch] = jnp.where(rows == 0, 0.0, pltpu.roll(u, 1, 0)).astype(BF16)
        u3[pl.ds(off, width), ch:2 * ch] = u.astype(BF16)
        u3[pl.ds(off, width), 2 * ch:3 * ch] = jnp.where(rows == width - 1, 0.0, pltpu.roll(u, width - 1, 0)).astype(BF16)

    prep(top_ref[...], 0, edge_ref[0] != 0)
    prep(bot_ref[...], n_rows + 1, edge_ref[1] != 0)
    for b in range(n_blk):
        x_in[b].wait()

        def prep_row(i, _):
            row = b * blk_rows + i
            prep(xs[pl.ds(pl.multiple_of(row * width, width), width), :], row + 1)
            return 0

        lax.fori_loop(0, blk_rows, prep_row, 0)
    for c in w_in:
        c.wait()
    if has_res:
        r_in.wait()
    st_ref[...] = jnp.zeros_like(st_ref)

    def block(b, _):
        off = pl.multiple_of(b * m, m)
        acc = jnp.dot(u3[pl.ds(off, m), :], ws[0], preferred_element_type=F32)
        acc += jnp.dot(u3[pl.ds(pl.multiple_of(off + width, width), m), :], ws[1], preferred_element_type=F32)
        acc += jnp.dot(u3[pl.ds(pl.multiple_of(off + 2 * width, width), m), :], ws[2], preferred_element_type=F32)
        acc += b_ref[...]
        if has_res:
            acc += rs[pl.ds(off, m), :].astype(F32)
        y = acc.astype(BF16)
        ys[pl.ds(off, m), :] = y
        yf = y.astype(F32)
        add_stats(st_ref, yf)
        pltpu.make_async_copy(ys.at[pl.ds(off, m)], y_ref.at[pl.ds(off, m)], y_sem.at[b]).start()
        return 0

    lax.fori_loop(0, n_blk, block, 0)
    for b in range(n_blk):
        pltpu.make_async_copy(ys.at[pl.ds(b * m, m)], y_ref.at[pl.ds(b * m, m)], y_sem.at[b]).wait()


def conv(width, x, top, bot, edge, aff, w3, bias, res=None):
    tok, ch = x.shape
    n_rows = tok // width
    blk_rows = 4
    n_blk = n_rows // blk_rows
    has_res = res is not None
    scratch = [
        pltpu.VMEM((tok, ch), BF16),
        pltpu.VMEM((tok + 2 * width, 3 * ch), BF16),
        pltpu.VMEM(w3.shape, BF16),
        pltpu.VMEM((tok, ch), BF16),
    ]
    sems = [pltpu.SemaphoreType.DMA((n_blk,)), pltpu.SemaphoreType.DMA((3,)), pltpu.SemaphoreType.DMA((n_blk,))]
    if has_res:
        scratch.append(pltpu.VMEM((tok, ch), BF16))
        sems.append(pltpu.SemaphoreType.DMA((1,)))
    args = [x, top, bot, edge, aff, w3, bias] + ([res] if has_res else [])
    return pl.pallas_call(
        functools.partial(conv_kernel, width, n_rows, blk_rows, has_res),
        out_shape=(jax.ShapeDtypeStruct((tok, ch), BF16), jax.ShapeDtypeStruct((16, ch), F32)),
        in_specs=[ANY, VMEM, VMEM, SMEM, VMEM, ANY, VMEM] + ([ANY] if has_res else []),
        out_specs=(ANY, VMEM),
        scratch_shapes=scratch + sems,
        name='conv_res' if has_res else 'conv',
        compiler_params=pltpu.CompilerParams(vmem_limit_bytes=48 * MIB),
    )(*args)


def attn_kernel(n_dev, n_chunk, q_blk, q_sub, h_ref, aff_ref, wq_ref, wk_ref, wv_ref, wo_ref, b_ref, y_ref, st_ref,
                nbuf, q_s, acc_s, m_s, l_s, k_s, v_s, send_sem, recv_sem):
    tok, ch = h_ref.shape
    kc = tok // n_chunk
    half = n_chunk // 2
    n_recv = 3 * n_chunk
    scale = ch ** -0.5 * LOG2E
    right, left = peer(n_dev, 1), peer(n_dev, -1)
    barrier = pltpu.get_barrier_semaphore()
    for p in (left, right):
        pl.semaphore_signal(barrier, inc=1, device_id=p, device_id_type=MESH)
    pl.semaphore_wait(barrier, 2)
    sends = []
    for i in range(n_chunk):
        for side, p in ((0, right), (1, left)):
            c = i if side == 0 else (i + half) % n_chunk
            slot = 2 * i + side
            sends.append(pltpu.make_async_remote_copy(
                h_ref.at[pl.ds(c * kc, kc)], nbuf.at[slot], send_sem.at[slot], recv_sem.at[slot], device_id=p, device_id_type=MESH))
    for c in sends:
        c.start()

    def forward(slot):
        return pltpu.make_async_remote_copy(
            nbuf.at[slot], nbuf.at[2 * n_chunk + slot], send_sem.at[2 * n_chunk + slot], recv_sem.at[2 * n_chunk + slot],
            device_id=right if slot % 2 == 0 else left, device_id_type=MESH)

    mean, gain, shift = aff_ref[0:1, :], aff_ref[8:9, :], aff_ref[16:17, :]

    def norm(v):
        return ((v.astype(F32) - mean) * gain + shift).astype(BF16)

    pb = 512

    def project_q(i, _):
        rows = pl.ds(pl.multiple_of(i * pb, pb), pb)
        q_s[rows, :] = (jnp.dot(norm(h_ref[rows, :]), wq_ref[...], preferred_element_type=F32) + b_ref[0:1, :]).astype(BF16)
        acc_s[rows, :] = jnp.zeros((pb, ch), F32)
        m_s[rows, :] = jnp.full((pb, 128), -jnp.inf, F32)
        l_s[rows, :] = jnp.zeros((pb, 128), F32)
        return 0

    lax.fori_loop(0, tok // pb, project_q, 0)

    def step(s, _):
        def project_kv(load):
            def body(i, _):
                rows = pl.ds(pl.multiple_of(i * pb, pb), pb)
                n = norm(load(i * pb))
                k_s[rows, :] = (jnp.dot(n, wk_ref[...], preferred_element_type=F32) + b_ref[1:2, :]).astype(BF16)
                v_s[rows, :] = (jnp.dot(n, wv_ref[...], preferred_element_type=F32) + b_ref[2:3, :]).astype(BF16)
                return 0
            lax.fori_loop(0, kc // pb, body, 0)

        @pl.when(s < n_chunk)
        def _():
            project_kv(lambda o: h_ref[pl.ds(pl.multiple_of(s * kc + o, pb), pb), :])

        @pl.when(s >= n_chunk)
        def _():
            slot = s - n_chunk
            pltpu.make_async_remote_copy(
                nbuf.at[slot], nbuf.at[slot], send_sem.at[slot], recv_sem.at[slot], device_id=right, device_id_type=MESH).wait_recv()
            for f in range(n_chunk):
                @pl.when(slot == f)
                def _():
                    forward(f).start()
            project_kv(lambda o: nbuf[slot, pl.ds(pl.multiple_of(o, pb), pb), :])

        def q_block(i, _):
            n_sub = q_blk // q_sub
            base = i * q_blk
            rows = [pl.ds(pl.multiple_of(base + j * q_sub, q_sub), q_sub) for j in range(n_sub)]

            def score(j):
                return lax.dot_general(q_s[rows[j], :], k_s[...], (((1,), (1,)), ((), ())), preferred_element_type=F32)

            def update(j, sc):
                m_old = m_s[rows[j], :]
                m_new = jnp.maximum(m_old, jnp.max(sc, axis=1, keepdims=True))
                alpha = jnp.exp2((m_old - m_new) * scale)
                p = jnp.exp2((sc - jnp.tile(m_new, (1, kc // 128))) * scale)
                part = p[:, 0:128]
                for t in range(1, kc // 128):
                    part = part + p[:, t * 128:(t + 1) * 128]
                l_s[rows[j], :] = l_s[rows[j], :] * alpha + part
                m_s[rows[j], :] = m_new
                pv = jnp.dot(p.astype(BF16), v_s[...], preferred_element_type=F32)
                acc_s[rows[j], :] = acc_s[rows[j], :] * jnp.tile(alpha, (1, ch // 128)) + pv

            sc = score(0)
            for j in range(n_sub):
                nxt = score(j + 1) if j + 1 < n_sub else None
                update(j, sc)
                sc = nxt
            return 0

        lax.fori_loop(0, tok // q_blk, q_block, 0)
        return 0

    lax.fori_loop(0, n_chunk + n_recv, step, 0)

    st_ref[...] = jnp.zeros_like(st_ref)

    def finish(i, _):
        rows = pl.ds(pl.multiple_of(i * pb, pb), pb)
        o = (acc_s[rows, :] / jnp.sum(l_s[rows, :], axis=1, keepdims=True)).astype(BF16)
        y = (h_ref[rows, :].astype(F32) + (jnp.dot(o, wo_ref[...], preferred_element_type=F32) + b_ref[3:4, :])).astype(BF16)
        y_ref[rows, :] = y
        yf = y.astype(F32)
        add_stats(st_ref, yf)
        return 0

    lax.fori_loop(0, tok // pb, finish, 0)
    for c in sends:
        c.wait_send()
    for f in range(n_chunk):
        forward(f).wait_send()


def attention(n_dev, h, aff, w_attn, b_attn):
    tok, ch = h.shape
    n_chunk = 4
    kc = tok // n_chunk
    n_recv = 3 * n_chunk
    return pl.pallas_call(
        functools.partial(attn_kernel, n_dev, n_chunk, 1024, 256),
        out_shape=(jax.ShapeDtypeStruct((tok, ch), BF16), jax.ShapeDtypeStruct((16, ch), F32)),
        in_specs=[VMEM] * 7,
        out_specs=(VMEM, VMEM),
        scratch_shapes=[
            pltpu.VMEM((n_recv, kc, ch), BF16),
            pltpu.VMEM((tok, ch), BF16),
            pltpu.VMEM((tok, ch), F32),
            pltpu.VMEM((tok, 128), F32),
            pltpu.VMEM((tok, 128), F32),
            pltpu.VMEM((kc, ch), BF16),
            pltpu.VMEM((kc, ch), BF16),
            pltpu.SemaphoreType.DMA((n_recv,)),
            pltpu.SemaphoreType.DMA((n_recv,)),
        ],
        name='attention',
        compiler_params=pltpu.CompilerParams(collective_id=1, has_side_effects=True, vmem_limit_bytes=63 * MIB),
    )(h, aff, w_attn[0], w_attn[1], w_attn[2], w_attn[3], b_attn)


def solution(mesh):
    n_dev = mesh.shape['cp']

    def local_fn(latents, w_in, b_in, w_conv, b_conv, gn_scale, gn_shift, w_attn, b_attn):
        _, band, width, z_ch = latents.shape
        ch = w_in.shape[3]
        n_rows = 2 * band
        tok = n_rows * width
        idx = lax.axis_index('cp')
        core = lax.rem(idx, 2)
        chip = idx // 2
        n_chip = n_dev // 2

        swap = [(i, i ^ 1) for i in range(n_dev)]
        mine = lax.dynamic_index_in_dim(latents, core, 0, keepdims=False)
        other = lax.ppermute(lax.dynamic_index_in_dim(latents, 1 - core, 0, keepdims=False), 'cp', swap)
        down = [lax.ppermute(latents[c, -1:], 'cp', [(2 * i + 1, 2 * (i + 1) + c) for i in range(n_chip - 1)]) for c in range(2)]
        up = [lax.ppermute(latents[c, :1], 'cp', [(2 * (i + 1), 2 * i + c) for i in range(n_chip - 1)]) for c in range(2)]
        first, second = jnp.where(core == 0, mine, other), jnp.where(core == 0, other, mine)
        rows = jnp.concatenate([down[0] + down[1], first, second, up[0] + up[1]], axis=0)
        rows = jnp.pad(jnp.transpose(rows, (2, 0, 1)), ((0, 0), (0, 0), (1, 1)))
        patches = jnp.concatenate([rows[:, dy:dy + n_rows, dx:dx + width] for dy in range(3) for dx in range(3)], axis=0)
        h, st = conv_in(patches.reshape(9 * z_ch, tok), w_in.reshape(9 * z_ch, ch), b_in.astype(F32).reshape(1, ch))

        edge = jnp.stack([chip > 0, chip < n_chip - 1]).astype(jnp.int32)
        gains = jnp.repeat(jnp.stack([gn_scale, gn_shift], axis=1).astype(F32), 8, axis=1)
        w3 = w_conv.reshape(w_conv.shape[0], 3, 3 * ch, ch)
        bc = b_conv.astype(F32)[:, None, :]

        def resnet(h, st, a, g):
            aff, top, bot = exchange(n_dev, width, h, st, gains[g])
            t, st = conv(width, h, top, bot, edge, aff, w3[a], bc[a])
            aff, top, bot = exchange(n_dev, width, t, st, gains[g + 1])
            return conv(width, t, top, bot, edge, aff, w3[a + 1], bc[a + 1], h)

        h, st = resnet(h, st, 0, 0)
        aff, _, _ = exchange(n_dev, width, h, st, gains[2])
        h, st = attention(n_dev, h, aff, w_attn, b_attn.astype(F32))
        h, _ = resnet(h, st, 2, 3)

        h = h.reshape(2, band, width, ch)
        keep = lax.dynamic_index_in_dim(h, core, 0, keepdims=False)
        got = lax.ppermute(lax.dynamic_index_in_dim(h, 1 - core, 0, keepdims=False), 'cp', swap)
        return jnp.stack([jnp.where(core == 0, keep, got), jnp.where(core == 0, got, keep)])

    band_spec = P('dp', 'cp')
    whole_spec = P()
    return jax.shard_map(local_fn, mesh=mesh, in_specs=(band_spec,) + (whole_spec,) * 8, out_specs=band_spec, check_vma=False)
```

```python
import functools

import jax
import jax.numpy as jnp
from jax import lax
from jax.experimental import pallas as pl
from jax.experimental.pallas import tpu as pltpu
from jax.sharding import PartitionSpec as P

GROUPS = 32
GN_EPS = 1e-6
LOG2E = 1.4426950408889634
MESH = pl.DeviceIdType.MESH
F32, BF16 = jnp.float32, jnp.bfloat16
ANY = pl.BlockSpec(memory_space=pl.ANY)
VMEM = pl.BlockSpec(memory_space=pltpu.VMEM)
SMEM = pl.BlockSpec(memory_space=pltpu.SMEM)
MIB = 1024 * 1024


def peer(n_dev, offset):
    return {'cp': lax.rem(lax.axis_index('cp') + 2 * offset + n_dev, n_dev)}


def add_stats(st_s, yf):
    y3 = yf.reshape(yf.shape[0] // 8, 8, yf.shape[1])
    st_s[0:8, :] += jnp.sum(y3, axis=0)
    st_s[8:16, :] += jnp.sum(y3 * y3, axis=0)


def fold_stats(st_s):
    a, b = st_s[0:8, :], st_s[8:16, :]
    row = lax.broadcasted_iota(jnp.int32, a.shape, 0)
    return jnp.where(row < 4, a + pltpu.roll(a, 4, 0), b + pltpu.roll(b, 4, 0))


def conv_in_kernel(n_blk, width, z_ref, w_ref, b_ref, y_ref, st_ref, p_s, st_s):
    tok = y_ref.shape[0]
    z_ch, span = z_ref.shape
    m = tok // n_blk
    z = z_ref[...].astype(F32)
    col = lax.rem(lax.broadcasted_iota(jnp.int32, z.shape, 1), width)
    taps = [jnp.where(col == 0, 0.0, pltpu.roll(z, 1, 1)), z, jnp.where(col == width - 1, 0.0, pltpu.roll(z, span - 1, 1))]
    for dx in range(3):
        tap = taps[dx].astype(BF16)
        for dy in range(3):
            k = (3 * dy + dx) * z_ch
            p_s[k:k + z_ch, :] = tap[:, dy * width:dy * width + tok]
    st_s[...] = jnp.zeros_like(st_s)

    def body(i, _):
        off = pl.multiple_of(i * m, m)
        acc = lax.dot_general(p_s[:, pl.ds(off, m)], w_ref[...], (((0,), (0,)), ((), ())), preferred_element_type=F32)
        y = (acc + b_ref[...]).astype(BF16)
        y_ref[pl.ds(off, m), :] = y
        add_stats(st_s, y.astype(F32))
        return 0

    lax.fori_loop(0, n_blk, body, 0)
    st_ref[...] = fold_stats(st_s)


def conv_in(width, z, w2, bias):
    tok, ch = z.shape[1] - 2 * width, w2.shape[1]
    return pl.pallas_call(
        functools.partial(conv_in_kernel, 8, width),
        out_shape=(jax.ShapeDtypeStruct((tok, ch), BF16), jax.ShapeDtypeStruct((8, ch), F32)),
        in_specs=[VMEM] * 3,
        out_specs=(VMEM, VMEM),
        scratch_shapes=[pltpu.VMEM((w2.shape[0], tok), BF16), pltpu.VMEM((16, ch), F32)],
        name='conv_in',
        compiler_params=pltpu.CompilerParams(vmem_limit_bytes=24 * MIB),
    )(z, w2, bias)


def greet_peers(n_dev):
    barrier = pltpu.get_barrier_semaphore()
    for d in range(1, n_dev // 2):
        pl.semaphore_signal(barrier, inc=1, device_id=peer(n_dev, d), device_id_type=MESH)


def await_peers(n_dev):
    pl.semaphore_wait(pltpu.get_barrier_semaphore(), n_dev // 2 - 1)


def share_scratch(n_dev, ch):
    n_peer = n_dev // 2 - 1
    return [pltpu.VMEM((n_peer, 8, ch), F32), pltpu.SemaphoreType.DMA((n_peer,)), pltpu.SemaphoreType.DMA((n_peer,))]


def exchange_kernel(n_dev, count, st_ref, gain_ref, aff_ref, sbuf, send_sem, recv_sem):
    greet_peers(n_dev)
    await_peers(n_dev)
    share_stats(n_dev, count, st_ref, gain_ref, aff_ref, sbuf, send_sem, recv_sem)


def share_stats(n_dev, count, st_ref, gain_ref, aff_ref, sbuf, send_sem, recv_sem):
    n_chip = n_dev // 2
    copies = [pltpu.make_async_remote_copy(
        st_ref, sbuf.at[d - 1], send_sem.at[d - 1], recv_sem.at[d - 1], device_id=peer(n_dev, d), device_id_type=MESH)
        for d in range(1, n_chip)]
    for c in copies:
        c.start()
    tot = st_ref[...]
    for c in copies:
        c.wait()
    for d in range(1, n_chip):
        tot = tot + sbuf[d - 1]
    ch = tot.shape[1]
    row = lax.broadcasted_iota(jnp.int32, tot.shape, 0)
    lane = lax.broadcasted_iota(jnp.int32, tot.shape, 1)
    for k in (1, 2):
        tot = tot + jnp.where((row & k) != 0, pltpu.roll(tot, k, 0), pltpu.roll(tot, 8 - k, 0))
    k = 1
    while k < ch // GROUPS:
        tot = tot + jnp.where((lane & k) != 0, pltpu.roll(tot, k, 1), pltpu.roll(tot, ch - k, 1))
        k *= 2
    tot = tot * (1.0 / count)
    flip = pltpu.roll(tot, 4, 0)
    mean, square = jnp.where(row < 4, tot, flip), jnp.where(row < 4, flip, tot)
    aff_ref[0:8, :] = mean
    aff_ref[8:16, :] = lax.rsqrt(square - mean * mean + GN_EPS) * gain_ref[0:8, :]
    aff_ref[16:24, :] = gain_ref[8:16, :]


def exchange(n_dev, tok, st, gain):
    ch = st.shape[1]
    n_chip = n_dev // 2
    count = tok * n_chip * (ch // GROUPS)
    return pl.pallas_call(
        functools.partial(exchange_kernel, n_dev, count),
        out_shape=jax.ShapeDtypeStruct((24, ch), F32),
        in_specs=[VMEM, VMEM],
        out_specs=VMEM,
        scratch_shapes=share_scratch(n_dev, ch),
        name='exchange',
        compiler_params=pltpu.CompilerParams(collective_id=0, has_side_effects=True, vmem_limit_bytes=8 * MIB),
    )(st, gain)


def conv_kernel(n_dev, width, n_rows, blk_rows, which, has_res, share, count, *refs):
    refs = list(refs)

    def take(n):
        got = refs[:n]
        del refs[:n]
        return got

    x_ref, aff_ref, w_ref, b_ref = take(4)
    r_ref, = take(1) if has_res else (None,)
    gain_ref, = take(1) if share else (None,)
    y_ref, = take(1)
    out_aff_ref, = take(1) if share else (None,)
    xs, ua, ub, ws, ys, st_s, own, x_sem, w_sem, y_sem, send_sem, recv_sem = take(12)
    rs, r_sem = take(2) if has_res else (None, None)
    tok, ch = x_ref.shape
    n_blk = n_rows // blk_rows
    m = blk_rows * width
    right, left = peer(n_dev, 1), peer(n_dev, -1)
    greet_peers(n_dev)
    x_in = [pltpu.make_async_copy(x_ref.at[pl.ds(b * m, m)], xs.at[pl.ds(width + b * m, m)], x_sem.at[b]) for b in range(n_blk)]
    for c in x_in:
        c.start()
    w_in = [pltpu.make_async_copy(w_ref.at[which, d], ws.at[d], w_sem.at[d]) for d in range(3)]
    for c in w_in:
        c.start()
    if has_res:
        r_in = pltpu.make_async_copy(r_ref, rs, r_sem.at[0])
        r_in.start()
    await_peers(n_dev)
    halos = [
        pltpu.make_async_remote_copy(x_ref.at[pl.ds(tok - width, width)], xs.at[pl.ds(0, width)],
                                     send_sem.at[0], recv_sem.at[0], device_id=right, device_id_type=MESH),
        pltpu.make_async_remote_copy(x_ref.at[pl.ds(0, width)], xs.at[pl.ds(width + tok, width)],
                                     send_sem.at[1], recv_sem.at[1], device_id=left, device_id_type=MESH),
    ]
    for c in halos:
        c.start()
    st_s[...] = jnp.zeros_like(st_s)
    mean, scale, shift = aff_ref[0:1, :], aff_ref[8:9, :], aff_ref[16:17, :]
    chip = lax.axis_index('cp') // 2
    has_top, has_bot = chip > 0, chip < n_dev // 2 - 1
    cols = lax.broadcasted_iota(jnp.int32, (width, ch), 0)

    def block_of(j):
        return lax.rem(j + 1, n_blk)

    def prep(u3, b):
        for r in range(blk_rows + 2):
            v = xs[pl.ds(pl.multiple_of((b * blk_rows + r) * width, width), width), :]
            t = (v.astype(F32) - mean) * scale + shift
            u = t / (1.0 + jnp.exp(-t))
            if r == 0:
                u = jnp.where(jnp.logical_or(b > 0, has_top), u, 0.0)
            if r == blk_rows + 1:
                u = jnp.where(jnp.logical_or(b < n_blk - 1, has_bot), u, 0.0)
            rows = slice(r * width, (r + 1) * width)
            u3[rows, 0:ch] = jnp.where(cols == 0, 0.0, pltpu.roll(u, 1, 0)).astype(BF16)
            u3[rows, ch:2 * ch] = u.astype(BF16)
            u3[rows, 2 * ch:3 * ch] = jnp.where(cols == width - 1, 0.0, pltpu.roll(u, width - 1, 0)).astype(BF16)

    def dots(u3, b):
        off = pl.multiple_of(b * m, m)
        acc = jnp.dot(u3[0:m, :], ws[0], preferred_element_type=F32)
        acc += jnp.dot(u3[width:width + m, :], ws[1], preferred_element_type=F32)
        acc += jnp.dot(u3[2 * width:2 * width + m, :], ws[2], preferred_element_type=F32)
        acc += b_ref[...]
        if has_res:
            acc += rs[pl.ds(off, m), :].astype(F32)
        y = acc.astype(BF16)
        ys[pl.ds(off, m), :] = y
        if share:
            add_stats(st_s, y.astype(F32))
        pltpu.make_async_copy(ys.at[pl.ds(off, m)], y_ref.at[pl.ds(off, m)], y_sem.at[b]).start()

    for c in x_in[:3]:
        c.wait()
    prep(ua, 1)
    for c in x_in[3:]:
        c.wait()
    for c in w_in:
        c.wait()
    if has_res:
        r_in.wait()

    def pair(i, _):
        @pl.when(i == n_blk // 2 - 2)
        def _():
            for c in halos:
                c.wait_recv()

        j = 2 * i
        dots(ua, block_of(j))
        prep(ub, block_of(j + 1))
        dots(ub, block_of(j + 1))
        prep(ua, block_of(j + 2))
        return 0

    lax.fori_loop(0, n_blk // 2, pair, 0)
    own[...] = fold_stats(st_s)
    for c in halos:
        c.wait_send()
    for b in range(n_blk):
        pltpu.make_async_copy(ys.at[pl.ds(b * m, m)], y_ref.at[pl.ds(b * m, m)], y_sem.at[b]).wait()
    if share:
        share_stats(n_dev, count, own, gain_ref, out_aff_ref, *refs)


def conv(n_dev, width, x, aff, w3, which, bias, res=None, gain=None):
    tok, ch = x.shape
    n_rows = tok // width
    blk_rows = 4
    n_blk = n_rows // blk_rows
    has_res, share = res is not None, gain is not None
    count = tok * (n_dev // 2) * (ch // GROUPS)
    scratch = [
        pltpu.VMEM((tok + 2 * width, ch), BF16),
        pltpu.VMEM(((blk_rows + 2) * width, 3 * ch), BF16),
        pltpu.VMEM(((blk_rows + 2) * width, 3 * ch), BF16),
        pltpu.VMEM(w3.shape[1:], BF16),
        pltpu.VMEM((tok, ch), BF16),
        pltpu.VMEM((16, ch), F32),
        pltpu.VMEM((8, ch), F32),
        pltpu.SemaphoreType.DMA((n_blk,)),
        pltpu.SemaphoreType.DMA((3,)),
        pltpu.SemaphoreType.DMA((n_blk,)),
        pltpu.SemaphoreType.DMA((2,)),
        pltpu.SemaphoreType.DMA((2,)),
    ]
    if has_res:
        scratch += [pltpu.VMEM((tok, ch), BF16), pltpu.SemaphoreType.DMA((1,))]
    if share:
        scratch += share_scratch(n_dev, ch)
    args = [x, aff, w3, bias] + ([res] if has_res else []) + ([gain] if share else [])
    out = pl.pallas_call(
        functools.partial(conv_kernel, n_dev, width, n_rows, blk_rows, which, has_res, share, count),
        out_shape=[jax.ShapeDtypeStruct((tok, ch), BF16)] + ([jax.ShapeDtypeStruct((24, ch), F32)] if share else []),
        in_specs=[ANY, VMEM, ANY, VMEM] + ([ANY] if has_res else []) + ([VMEM] if share else []),
        out_specs=[ANY] + ([VMEM] if share else []),
        scratch_shapes=scratch,
        name=f'conv_{which}',
        compiler_params=pltpu.CompilerParams(
            collective_id=2 + which, has_side_effects=True, vmem_limit_bytes=63 * MIB),
    )(*args)
    return out if share else out[0]


def attn_kernel(n_dev, n_chunk, q_blk, q_sub, count, h_ref, aff_ref, w_ref, b_ref, gain_ref, y_ref, out_aff_ref,
                nbuf, q_s, acc_s, m_s, l_s, k_s, v_s, ys, st_s, own, send_sem, recv_sem, y_sem, *share_refs):
    tok, ch = h_ref.shape
    kc = tok // n_chunk
    half = n_chunk // 2
    n_recv = 3 * n_chunk
    scale = ch ** -0.5 * LOG2E
    right, left = peer(n_dev, 1), peer(n_dev, -1)
    greet_peers(n_dev)
    await_peers(n_dev)
    sends = []
    for i in range(n_chunk):
        for side, p in ((0, right), (1, left)):
            c = i if side == 0 else (i + half) % n_chunk
            slot = 2 * i + side
            sends.append(pltpu.make_async_remote_copy(
                h_ref.at[pl.ds(c * kc, kc)], nbuf.at[slot], send_sem.at[slot], recv_sem.at[slot], device_id=p, device_id_type=MESH))

    def forward(slot):
        return pltpu.make_async_remote_copy(
            nbuf.at[slot], nbuf.at[2 * n_chunk + slot], send_sem.at[2 * n_chunk + slot], recv_sem.at[2 * n_chunk + slot],
            device_id=right if slot % 2 == 0 else left, device_id_type=MESH)

    events = {0: sends[0:2], 1: sends[2:4]}
    for i in range(2, n_chunk):
        events[2 * i - 1] = sends[2 * i:2 * i + 2]
    for i in range(half):
        events[2 * n_chunk - 1 + 2 * i] = [forward(2 * i), forward(2 * i + 1)]

    mean, gain, shift = aff_ref[0:1, :], aff_ref[8:9, :], aff_ref[16:17, :]

    def norm(v):
        return ((v.astype(F32) - mean) * gain + shift).astype(BF16)

    pb = min(512, kc)
    for c in events[0]:
        c.start()

    def project_q(i, _):
        rows = pl.ds(pl.multiple_of(i * pb, pb), pb)
        q_s[rows, :] = (jnp.dot(norm(h_ref[rows, :]), w_ref[0], preferred_element_type=F32) + b_ref[0:1, :]).astype(BF16)
        acc_s[rows, :] = jnp.zeros((pb, ch), F32)
        m_s[rows, :] = jnp.full((pb, 128), -jnp.inf, F32)
        l_s[rows, :] = jnp.zeros((pb, 128), F32)
        return 0

    lax.fori_loop(0, tok // pb, project_q, 0)

    def step(s, _):
        for at, group in events.items():
            if at == 0:
                continue

            @pl.when(s == at)
            def _():
                for c in group:
                    c.start()

        def project_kv(load):
            def body(i, _):
                rows = pl.ds(pl.multiple_of(i * pb, pb), pb)
                n = norm(load(i * pb))
                k_s[rows, :] = (jnp.dot(n, w_ref[1], preferred_element_type=F32) + b_ref[1:2, :]).astype(BF16)
                v_s[rows, :] = (jnp.dot(n, w_ref[2], preferred_element_type=F32) + b_ref[2:3, :]).astype(BF16)
                return 0
            lax.fori_loop(0, kc // pb, body, 0)

        @pl.when(s < n_chunk)
        def _():
            project_kv(lambda o: h_ref[pl.ds(pl.multiple_of(s * kc + o, pb), pb), :])

        @pl.when(s >= n_chunk)
        def _():
            slot = s - n_chunk
            pltpu.make_async_remote_copy(
                nbuf.at[slot], nbuf.at[slot], send_sem.at[slot], recv_sem.at[slot], device_id=right, device_id_type=MESH).wait_recv()
            project_kv(lambda o: nbuf[slot, pl.ds(pl.multiple_of(o, pb), pb), :])

        def q_block(i, _):
            n_sub = q_blk // q_sub
            base = i * q_blk
            rows = [pl.ds(pl.multiple_of(base + j * q_sub, q_sub), q_sub) for j in range(n_sub)]

            def score(j):
                return lax.dot_general(q_s[rows[j], :], k_s[...], (((1,), (1,)), ((), ())), preferred_element_type=F32)

            def update(j, sc):
                m_old = m_s[rows[j], :]
                m_new = jnp.maximum(m_old, jnp.max(sc, axis=1, keepdims=True))
                alpha = jnp.exp2((m_old - m_new) * scale)
                p = jnp.exp2((sc - jnp.tile(m_new, (1, kc // 128))) * scale)
                part = p[:, 0:128]
                for t in range(1, kc // 128):
                    part = part + p[:, t * 128:(t + 1) * 128]
                l_s[rows[j], :] = l_s[rows[j], :] * alpha + part
                m_s[rows[j], :] = m_new
                pv = jnp.dot(p.astype(BF16), v_s[...], preferred_element_type=F32)
                acc_s[rows[j], :] = acc_s[rows[j], :] * jnp.tile(alpha, (1, ch // 128)) + pv

            sc = score(0)
            for j in range(n_sub):
                nxt = score(j + 1) if j + 1 < n_sub else None
                update(j, sc)
                sc = nxt
            return 0

        lax.fori_loop(0, tok // q_blk, q_block, 0)
        return 0

    lax.fori_loop(0, n_chunk + n_recv, step, 0)

    st_s[...] = jnp.zeros_like(st_s)

    def finish(i, _):
        rows = pl.ds(pl.multiple_of(i * pb, pb), pb)
        o = (acc_s[rows, :] / jnp.sum(l_s[rows, :], axis=1, keepdims=True)).astype(BF16)
        y = (h_ref[rows, :].astype(F32) + (jnp.dot(o, w_ref[3], preferred_element_type=F32) + b_ref[3:4, :])).astype(BF16)
        ys[rows, :] = y
        add_stats(st_s, y.astype(F32))
        pltpu.make_async_copy(ys.at[rows], y_ref.at[rows], y_sem.at[i]).start()
        return 0

    lax.fori_loop(0, tok // pb, finish, 0)
    own[...] = fold_stats(st_s)
    for i in range(tok // pb):
        rows = pl.ds(i * pb, pb)
        pltpu.make_async_copy(ys.at[rows], y_ref.at[rows], y_sem.at[i]).wait()
    for c in sends:
        c.wait_send()
    for f in range(n_chunk):
        forward(f).wait_send()
    share_stats(n_dev, count, own, gain_ref, out_aff_ref, *share_refs)


def attention(n_dev, h, aff, w_attn, b_attn, gain):
    tok, ch = h.shape
    n_chunk = 4
    kc = tok // n_chunk
    n_recv = 3 * n_chunk
    return pl.pallas_call(
        functools.partial(attn_kernel, n_dev, n_chunk, 1024, 512, tok * (n_dev // 2) * (ch // GROUPS)),
        out_shape=(jax.ShapeDtypeStruct((tok, ch), BF16), jax.ShapeDtypeStruct((24, ch), F32)),
        in_specs=[VMEM] * 5,
        out_specs=(ANY, VMEM),
        scratch_shapes=[
            pltpu.VMEM((n_recv, kc, ch), BF16),
            pltpu.VMEM((tok, ch), BF16),
            pltpu.VMEM((tok, ch), F32),
            pltpu.VMEM((tok, 128), F32),
            pltpu.VMEM((tok, 128), F32),
            pltpu.VMEM((kc, ch), BF16),
            pltpu.VMEM((kc, ch), BF16),
            pltpu.VMEM((tok, ch), BF16),
            pltpu.VMEM((16, ch), F32),
            pltpu.VMEM((8, ch), F32),
            pltpu.SemaphoreType.DMA((n_recv,)),
            pltpu.SemaphoreType.DMA((n_recv,)),
            pltpu.SemaphoreType.DMA((tok // min(512, kc),)),
        ] + share_scratch(n_dev, ch),
        name='attention',
        compiler_params=pltpu.CompilerParams(collective_id=1, has_side_effects=True, vmem_limit_bytes=63 * MIB),
    )(h, aff, w_attn, b_attn, gain)


def solution(mesh):
    n_dev = mesh.shape['cp']

    def local_fn(latents, w_in, b_in, w_conv, b_conv, gn_scale, gn_shift, w_attn, b_attn):
        _, band, width, z_ch = latents.shape
        ch = w_in.shape[3]
        n_rows = 2 * band
        tok = n_rows * width
        idx = lax.axis_index('cp')
        core = lax.rem(idx, 2)
        n_chip = n_dev // 2

        swap = [(i, i ^ 1) for i in range(n_dev)]
        mine = lax.dynamic_index_in_dim(latents, core, 0, keepdims=False)
        other = lax.ppermute(lax.dynamic_index_in_dim(latents, 1 - core, 0, keepdims=False), 'cp', swap)
        down = [lax.ppermute(latents[c, -1:], 'cp', [(2 * i + 1, 2 * (i + 1) + c) for i in range(n_chip - 1)]) for c in range(2)]
        up = [lax.ppermute(latents[c, :1], 'cp', [(2 * (i + 1), 2 * i + c) for i in range(n_chip - 1)]) for c in range(2)]
        first, second = jnp.where(core == 0, mine, other), jnp.where(core == 0, other, mine)
        rows = jnp.concatenate([down[0] + down[1], first, second, up[0] + up[1]], axis=0)
        z = jnp.transpose(rows.reshape(tok + 2 * width, z_ch), (1, 0))
        h, st = conv_in(width, z, w_in.reshape(9 * z_ch, ch), b_in.astype(F32).reshape(1, ch))

        gains = jnp.repeat(jnp.stack([gn_scale, gn_shift], axis=1).astype(F32), 8, axis=1)
        w3 = w_conv.reshape(w_conv.shape[0], 3, 3 * ch, ch)
        bc = b_conv.astype(F32)[:, None, :]

        def resnet(h, aff, a, g, gain=None):
            t, aff = conv(n_dev, width, h, aff, w3, a, bc[a], None, gains[g + 1])
            return conv(n_dev, width, t, aff, w3, a + 1, bc[a + 1], h, gain)

        aff = exchange(n_dev, tok, st, gains[0])
        h, aff = resnet(h, aff, 0, 0, gains[2])
        h, aff = attention(n_dev, h, aff, w_attn, b_attn.astype(F32), gains[3])
        h = resnet(h, aff, 2, 3)

        h = h.reshape(2, band, width, ch)
        keep = lax.dynamic_index_in_dim(h, core, 0, keepdims=False)
        got = lax.ppermute(lax.dynamic_index_in_dim(h, 1 - core, 0, keepdims=False), 'cp', swap)
        return jnp.stack([jnp.where(core == 0, keep, got), jnp.where(core == 0, got, keep)])

    band_spec = P('dp', 'cp')
    whole_spec = P()
    return jax.shard_map(local_fn, mesh=mesh, in_specs=(band_spec,) + (whole_spec,) * 8, out_specs=band_spec, check_vma=False)
```
